8 devices in a mesh: dp: 1 (over z), cp: 8 (over y, x, core).
Axes of the slice: x: 2, y: 2, z: 1, core: 2. Of those that a mesh axis runs over, the one named last changes fastest.
Arguments:
- queries: bfloat16 [3, 3072, 32, 128], P('dp', 'cp')
- keys: bfloat16 [3, 3072, 16, 128], P('dp', 'cp')
- values: bfloat16 [3, 3072, 16, 128], P('dp', 'cp')
- out_grad: bfloat16 [3, 3072, 32, 128], P('dp', 'cp')
Outputs:
- output 1: bfloat16 [3, 3072, 32, 128], P('dp', 'cp')
- output 2: float32 [3, 32, 3072], P('dp', None, 'cp')
- output 3: bfloat16 [3, 3072, 32, 128], P('dp', 'cp')
- output 4: bfloat16 [3, 3072, 16, 128], P('dp', 'cp')
- output 5: bfloat16 [3, 3072, 16, 128], P('dp', 'cp')
All inputs are finite; a program needn't handle non-finite values.
Results may differ from the reference program's by a relative error of at most 0.0187816.
Values are sent between devices in bfloat16 or wider.
A program may use at most 1 GiB of HBM per device.

```python
import jax
import jax.numpy as jnp
from jax import lax

BATCH = 3
SEQ = 3072
HEADS = 32
KV_HEADS = 16
HEAD = 128
QBLOCK = 128

RATIO = HEADS // KV_HEADS
SCALE = HEAD ** -0.5
NUM_BLOCKS = SEQ // QBLOCK


def setup_inputs(seed: int = 0, part: int = 0) -> dict:
    base_key = jax.random.fold_in(jax.random.key(seed), part)
    rng_keys = jax.random.split(base_key, 4)
    q_shape = (BATCH, SEQ, HEADS, HEAD)
    kv_shape = (BATCH, SEQ, KV_HEADS, HEAD)
    queries = jax.random.normal(rng_keys[0], q_shape, jnp.float32).astype(jnp.bfloat16)
    keys = jax.random.normal(rng_keys[1], kv_shape, jnp.float32).astype(jnp.bfloat16)
    values = jax.random.normal(rng_keys[2], kv_shape, jnp.float32).astype(jnp.bfloat16)
    out_grad = jax.random.normal(rng_keys[3], q_shape, jnp.float32).astype(jnp.bfloat16)
    return {"queries": queries, "keys": keys, "values": values, "out_grad": out_grad}


def reference(queries, keys, values, out_grad):
    keys_f = keys.astype(jnp.float32)
    values_f = values.astype(jnp.float32)
    key_pos = jnp.arange(SEQ)
    query_blocks = jnp.moveaxis(queries.reshape(BATCH, NUM_BLOCKS, QBLOCK, KV_HEADS, RATIO, HEAD), 1, 0)
    grad_blocks = jnp.moveaxis(out_grad.reshape(BATCH, NUM_BLOCKS, QBLOCK, KV_HEADS, RATIO, HEAD), 1, 0)

    def block_step(carry, block_in):
        grad_key, grad_value = carry
        block_idx, query_blk, grad_blk = block_in
        query_f = query_blk.astype(jnp.float32)
        grad_f = grad_blk.astype(jnp.float32)
        query_pos = block_idx * QBLOCK + jnp.arange(QBLOCK)
        causal = query_pos[:, None] >= key_pos[None, :]
        scores = jnp.einsum("bqgrd,bkgd->bgrqk", query_f, keys_f) * SCALE
        scores = jnp.where(causal, scores, -jnp.inf)
        row_max = jnp.max(scores, axis=-1, keepdims=True)
        row_lse = row_max + jnp.log(jnp.sum(jnp.exp(scores - row_max), axis=-1, keepdims=True))
        prob_mat = jnp.exp(scores - row_lse)
        prob_round = prob_mat.astype(jnp.bfloat16).astype(jnp.float32)
        out_blk = jnp.einsum("bgrqk,bkgd->bqgrd", prob_round, values_f).astype(jnp.bfloat16)
        delta = jnp.einsum("bqgrd,bqgrd->bgrq", grad_f, out_blk.astype(jnp.float32))
        grad_prob = jnp.einsum("bqgrd,bkgd->bgrqk", grad_f, values_f)
        grad_score = prob_mat * (grad_prob - delta[..., None])
        score_round = grad_score.astype(jnp.bfloat16).astype(jnp.float32)
        grad_query = jnp.einsum("bgrqk,bkgd->bqgrd", score_round, keys_f) * SCALE
        grad_key = grad_key + jnp.einsum("bgrqk,bqgrd->bkgd", score_round, query_f) * SCALE
        grad_value = grad_value + jnp.einsum("bgrqk,bqgrd->bkgd", prob_round, grad_f)
        return (grad_key, grad_value), (out_blk, row_lse[..., 0], grad_query.astype(jnp.bfloat16))

    zero_kv = jnp.zeros((BATCH, SEQ, KV_HEADS, HEAD), jnp.float32)
    carry_out, block_outs = lax.scan(block_step, (zero_kv, zero_kv), (jnp.arange(NUM_BLOCKS), query_blocks, grad_blocks))
    out_blocks, lse_blocks, dq_blocks = block_outs
    attn_out = jnp.moveaxis(out_blocks, 0, 1).reshape(BATCH, SEQ, HEADS, HEAD)
    row_lse = jnp.moveaxis(lse_blocks, 0, 3).reshape(BATCH, HEADS, SEQ)
    grad_query = jnp.moveaxis(dq_blocks, 0, 1).reshape(BATCH, SEQ, HEADS, HEAD)
    grad_key = carry_out[0].astype(jnp.bfloat16)
    grad_value = carry_out[1].astype(jnp.bfloat16)
    return attn_out, row_lse, grad_query, grad_key, grad_value
```

```python
import jax
import jax.numpy as jnp
from jax import lax
from jax.experimental import pallas as pl
from jax.experimental.pallas import tpu as pltpu
from jax.sharding import PartitionSpec as P


LOG2E = 1.4426950408889634
BQ = 256
BK = 512
TB = 64


def dot_nt(lhs, rhs):
    return lax.dot_general(lhs, rhs, (((1,), (1,)), ((), ())), preferred_element_type=jnp.float32)


def dot_nn(lhs, rhs):
    return lax.dot_general(lhs, rhs, (((1,), (0,)), ((), ())), preferred_element_type=jnp.float32)


def attention_kernel(x_ref, y_ref, lse_ref, q_cat, g_cat, k_t, v_t, s_buf, ot_acc, dqt_acc, dk_acc, dv_acc):
    seq = x_ref.shape[0]
    dim = k_t.shape[0]
    width = 2 * BQ
    scale = dim ** -0.5
    scale2 = scale * LOG2E
    q_col, g_col, k_col, v_col = 0, 2 * dim, 4 * dim, 5 * dim

    def prepare(blk, carry):
        rows = pl.ds(pl.multiple_of(blk * BK, BK), BK)
        k_t[:, rows] = x_ref[rows, k_col:k_col + dim].T
        v_t[:, rows] = x_ref[rows, v_col:v_col + dim].T
        dk_acc[rows, :] = jnp.zeros((BK, dim), jnp.float32)
        dv_acc[rows, :] = jnp.zeros((BK, dim), jnp.float32)
        return carry

    lax.fori_loop(0, seq // BK, prepare, 0)

    def fold(tile, op):
        return op(tile.reshape(BK // 8, 8, width), axis=0)

    def query_block(blk, carry):
        rows = pl.ds(pl.multiple_of(blk * BQ, BQ), BQ)
        for head in range(2):
            q_cat[head * BQ:(head + 1) * BQ, :] = x_ref[rows, q_col + head * dim:q_col + (head + 1) * dim]
            g_cat[head * BQ:(head + 1) * BQ, :] = x_ref[rows, g_col + head * dim:g_col + (head + 1) * dim]
        last = (blk * BQ) // BK

        def key_rows(step):
            return pl.ds(pl.multiple_of(step * BK, BK), BK)

        def score_step(step, run_max):
            scores = dot_nt(x_ref[key_rows(step), k_col:k_col + dim], q_cat[...])
            s_buf[key_rows(step), :] = scores
            return jnp.maximum(run_max, fold(scores, jnp.max))

        run_max = lax.fori_loop(0, last, score_step, jnp.full((8, width), -jnp.inf, jnp.float32))
        scores = dot_nt(x_ref[key_rows(last), k_col:k_col + dim], q_cat[...])
        key_pos = last * BK + lax.broadcasted_iota(jnp.int32, (BK, width), 0)
        query_pos = blk * BQ + lax.broadcasted_iota(jnp.int32, (BK, width), 1) % BQ
        scores = jnp.where(key_pos <= query_pos, scores, -jnp.inf)
        s_buf[key_rows(last), :] = scores
        run_max = jnp.maximum(run_max, fold(scores, jnp.max))
        row_max = jnp.max(run_max, axis=0, keepdims=True)
        shift = row_max * scale2
        ot_acc[...] = jnp.zeros_like(ot_acc)

        def value_step(step, run_sum):
            weights = jnp.exp2(s_buf[key_rows(step), :] * scale2 - shift)
            ot_acc[...] += dot_nn(v_t[:, key_rows(step)], weights.astype(jnp.bfloat16))
            return run_sum + fold(weights, jnp.sum)

        run_sum = lax.fori_loop(0, last + 1, value_step, jnp.zeros((8, width), jnp.float32))
        row_sum = jnp.sum(run_sum, axis=0, keepdims=True)
        out_t = (ot_acc[...] / row_sum).astype(jnp.bfloat16)
        row_lse = row_max * scale + jnp.log(row_sum)
        lse2 = row_lse * LOG2E
        out_f = out_t.astype(jnp.float32)
        grad_t = g_cat[...].astype(jnp.float32).T
        delta = jnp.sum(out_f * grad_t, axis=0, keepdims=True)
        out_n = out_f.T.astype(jnp.bfloat16)
        for head in range(2):
            y_ref[rows, head * dim:(head + 1) * dim] = out_n[head * BQ:(head + 1) * BQ, :]
            lse_ref[0, head:head + 1, rows] = row_lse[:, head * BQ:(head + 1) * BQ]
        dqt_acc[...] = jnp.zeros_like(dqt_acc)

        def grad_step(step, inner):
            probs = jnp.exp2(s_buf[key_rows(step), :] * scale2 - lse2)
            grad_prob = dot_nt(x_ref[key_rows(step), v_col:v_col + dim], g_cat[...])
            grad_score = (probs * (grad_prob - delta)).astype(jnp.bfloat16)
            dv_acc[key_rows(step), :] += dot_nn(probs.astype(jnp.bfloat16), g_cat[...])
            dk_acc[key_rows(step), :] += dot_nn(grad_score, q_cat[...])
            dqt_acc[...] += dot_nn(k_t[:, key_rows(step)], grad_score)
            return inner

        lax.fori_loop(0, last + 1, grad_step, 0)
        dq_n = (dqt_acc[...] * scale).T.astype(jnp.bfloat16)
        for head in range(2):
            y_ref[rows, (2 + head) * dim:(3 + head) * dim] = dq_n[head * BQ:(head + 1) * BQ, :]
        return carry

    lax.fori_loop(0, seq // BQ, query_block, 0)

    def finish(blk, carry):
        rows = pl.ds(pl.multiple_of(blk * BK, BK), BK)
        y_ref[rows, 4 * dim:5 * dim] = (dk_acc[rows, :] * scale).astype(jnp.bfloat16)
        y_ref[rows, 5 * dim:6 * dim] = dv_acc[rows, :].astype(jnp.bfloat16)
        return carry

    lax.fori_loop(0, seq // BK, finish, 0)


def attention_call(packed, groups, dim):
    seq = packed.shape[0]
    wide = 6 * dim
    pairs = groups * 2 * seq * seq // 2
    return pl.pallas_call(
        attention_kernel,
        grid=(groups,),
        in_specs=[pl.BlockSpec((seq, wide), lambda g: (0, g))],
        out_specs=[pl.BlockSpec((seq, wide), lambda g: (0, g)), pl.BlockSpec((1, 2, seq), lambda g: (g, 0, 0))],
        out_shape=[jax.ShapeDtypeStruct((seq, groups * wide), jnp.bfloat16), jax.ShapeDtypeStruct((groups, 2, seq), jnp.float32)],
        scratch_shapes=[
            pltpu.VMEM((2 * BQ, dim), jnp.bfloat16),
            pltpu.VMEM((2 * BQ, dim), jnp.bfloat16),
            pltpu.VMEM((dim, seq), jnp.bfloat16),
            pltpu.VMEM((dim, seq), jnp.bfloat16),
            pltpu.VMEM((seq, 2 * BQ), jnp.float32),
            pltpu.VMEM((dim, 2 * BQ), jnp.float32),
            pltpu.VMEM((dim, 2 * BQ), jnp.float32),
            pltpu.VMEM((seq, dim), jnp.float32),
            pltpu.VMEM((seq, dim), jnp.float32),
        ],
        compiler_params=pltpu.CompilerParams(dimension_semantics=("arbitrary",), vmem_limit_bytes=60 * 1024 * 1024),
        cost_estimate=pl.CostEstimate(flops=pairs * dim * 2 * 12, bytes_accessed=packed.size * 4, transcendentals=pairs * 2),
    )(packed)


def pack_kernel(q_ref, g_ref, k_ref, v_ref, o_ref):
    parts, _ = o_ref.shape[:2]
    dim = q_ref.shape[-1]
    groups = k_ref.shape[2] // parts
    wide = 6 * dim
    for ref, first, count in ((q_ref, 0, 2), (g_ref, 2, 2), (k_ref, 4, 1), (v_ref, 5, 1)):
        by_head = pltpu.einshape("thd->htd", ref[0])
        for head in range(ref.shape[2]):
            part, local = divmod(head, groups * count)
            group, lane = divmod(local, count)
            start = group * wide + (first + lane) * dim
            o_ref[part, :, start:start + dim] = by_head[head]


def pack_call(queries, out_grad, keys, values, idx, parts):
    _, tokens, heads, dim = queries.shape
    kv_heads = keys.shape[2]
    width = kv_heads // parts * 6 * dim
    big = pl.BlockSpec((1, TB, heads, dim), lambda i: (idx, i, 0, 0))
    small = pl.BlockSpec((1, TB, kv_heads, dim), lambda i: (idx, i, 0, 0))
    return pl.pallas_call(
        pack_kernel,
        grid=(tokens // TB,),
        in_specs=[big, big, small, small],
        out_specs=pl.BlockSpec((parts, TB, width), lambda i: (0, i, 0)),
        out_shape=jax.ShapeDtypeStruct((parts, tokens, width), jnp.bfloat16),
        compiler_params=pltpu.CompilerParams(dimension_semantics=("arbitrary",), vmem_limit_bytes=62 * 1024 * 1024),
        cost_estimate=pl.CostEstimate(flops=parts * tokens * width * 200, bytes_accessed=parts * tokens * width * 4, transcendentals=0),
    )(queries, out_grad, keys, values)


def unpack_kernel(*refs):
    y_ref = refs[0]
    o_ref, dq_ref, dk_ref, dv_ref = refs[-4:]
    parts = y_ref.shape[0]
    dim = o_ref.shape[-1]
    groups = dk_ref.shape[2] // parts
    wide = 6 * dim
    for ref, first, count in ((o_ref, 0, 2), (dq_ref, 2, 2), (dk_ref, 4, 1), (dv_ref, 5, 1)):
        rows = []
        for head in range(ref.shape[2]):
            part, local = divmod(head, groups * count)
            group, lane = divmod(local, count)
            start = group * wide + (first + lane) * dim
            rows.append(y_ref[part, :, start:start + dim])
        ref[0] = pltpu.einshape("htd->thd", jnp.stack(rows))


def unpack_call(y, prev, idx, batch, heads, kv_heads, dim):
    parts, tokens, width = y.shape
    big = pl.BlockSpec((1, TB, heads, dim), lambda i: (idx, i, 0, 0))
    small = pl.BlockSpec((1, TB, kv_heads, dim), lambda i: (idx, i, 0, 0))
    big_shape = jax.ShapeDtypeStruct((batch, tokens, heads, dim), jnp.bfloat16)
    small_shape = jax.ShapeDtypeStruct((batch, tokens, kv_heads, dim), jnp.bfloat16)
    return pl.pallas_call(
        unpack_kernel,
        grid=(tokens // TB,),
        in_specs=[pl.BlockSpec((parts, TB, width), lambda i: (0, i, 0))] + [pl.BlockSpec(memory_space=pl.ANY)] * len(prev),
        out_specs=[big, big, small, small],
        out_shape=[big_shape, big_shape, small_shape, small_shape],
        input_output_aliases={i + 1: i for i in range(len(prev))},
        compiler_params=pltpu.CompilerParams(dimension_semantics=("arbitrary",), vmem_limit_bytes=62 * 1024 * 1024),
        cost_estimate=pl.CostEstimate(flops=y.size * 200, bytes_accessed=y.size * 4, transcendentals=0),
    )(y, *prev)


def solution(mesh):
    cp_size = mesh.shape["cp"]

    def attention_shard(queries, keys, values, out_grad):
        batch, tokens, heads, dim = queries.shape
        kv_heads = keys.shape[2]
        groups = kv_heads // cp_size
        width = groups * 6 * dim
        ready, sums = [], []
        for idx in range(batch):
            packed = pack_call(queries, out_grad, keys, values, idx, cp_size)
            if idx:
                packed, ready[-1] = lax.optimization_barrier((packed, ready[-1]))
            ready.append(lax.all_to_all(packed, "cp", 0, 0, tiled=True))
        done = []
        for idx in range(batch):
            y, lse = attention_call(ready[idx].reshape(cp_size * tokens, width), groups, dim)
            y = y.reshape(cp_size, tokens, width)
            if idx:
                y, done[-1] = lax.optimization_barrier((y, done[-1]))
            done.append(lax.all_to_all(y, "cp", 0, 0, tiled=True))
            sums.append(lse)
        outs = ()
        for idx in range(batch):
            outs = unpack_call(done[idx], outs, idx, batch, heads, kv_heads, dim)
        lse = jnp.stack(sums).reshape(batch, groups * 2, cp_size, tokens)
        lse = lax.all_to_all(jnp.transpose(lse, (2, 0, 1, 3)), "cp", 0, 0, tiled=True)
        lse = jnp.transpose(lse, (1, 0, 2, 3)).reshape(batch, heads, tokens)
        return outs[0], lse, outs[1], outs[2], outs[3]

    seq_spec = P("dp", "cp")
    return jax.shard_map(attention_shard, mesh=mesh, in_specs=(seq_spec, seq_spec, seq_spec, seq_spec), out_specs=(seq_spec, P("dp", None, "cp"), seq_spec, seq_spec, seq_spec), check_vma=False)
```

```python
import jax
import jax.numpy as jnp
from jax import lax
from jax.experimental import pallas as pl
from jax.experimental.pallas import tpu as pltpu
from jax.sharding import PartitionSpec as P


LOG2E = 1.4426950408889634
BQ = 256
BK = 512
TB = 64


def dot_nt(lhs, rhs):
    return lax.dot_general(lhs, rhs, (((1,), (1,)), ((), ())), preferred_element_type=jnp.float32)


def dot_nn(lhs, rhs):
    return lax.dot_general(lhs, rhs, (((1,), (0,)), ((), ())), preferred_element_type=jnp.float32)


def attention_kernel(x_ref, *refs):
    y_ref, lse_ref, q_cat, g_cat, k_t, v_t, s_buf, ot_acc, dqt_acc, dk_acc, dv_acc = refs[-11:]
    seq = x_ref.shape[0]
    dim = k_t.shape[0]
    width = 2 * BQ
    scale = dim ** -0.5
    scale2 = scale * LOG2E
    q_col, g_col, k_col, v_col = 0, 2 * dim, 4 * dim, 5 * dim

    def prepare(blk, carry):
        rows = pl.ds(pl.multiple_of(blk * BK, BK), BK)
        k_t[:, rows] = x_ref[rows, k_col:k_col + dim].T
        v_t[:, rows] = x_ref[rows, v_col:v_col + dim].T
        dk_acc[rows, :] = jnp.zeros((BK, dim), jnp.float32)
        dv_acc[rows, :] = jnp.zeros((BK, dim), jnp.float32)
        return carry

    lax.fori_loop(0, seq // BK, prepare, 0)

    def fold(tile, op):
        return op(tile.reshape(BK // 8, 8, width), axis=0)

    def query_block(blk, carry):
        rows = pl.ds(pl.multiple_of(blk * BQ, BQ), BQ)
        for head in range(2):
            q_cat[head * BQ:(head + 1) * BQ, :] = x_ref[rows, q_col + head * dim:q_col + (head + 1) * dim]
            g_cat[head * BQ:(head + 1) * BQ, :] = x_ref[rows, g_col + head * dim:g_col + (head + 1) * dim]
        last = (blk * BQ) // BK

        def key_rows(step):
            return pl.ds(pl.multiple_of(step * BK, BK), BK)

        def score_step(step, run_max):
            scores = dot_nt(x_ref[key_rows(step), k_col:k_col + dim], q_cat[...])
            s_buf[key_rows(step), :] = scores
            return jnp.maximum(run_max, fold(scores, jnp.max))

        run_max = lax.fori_loop(0, last, score_step, jnp.full((8, width), -jnp.inf, jnp.float32))
        scores = dot_nt(x_ref[key_rows(last), k_col:k_col + dim], q_cat[...])
        key_pos = last * BK + lax.broadcasted_iota(jnp.int32, (BK, width), 0)
        query_pos = blk * BQ + lax.broadcasted_iota(jnp.int32, (BK, width), 1) % BQ
        scores = jnp.where(key_pos <= query_pos, scores, -jnp.inf)
        s_buf[key_rows(last), :] = scores
        run_max = jnp.maximum(run_max, fold(scores, jnp.max))
        row_max = jnp.max(run_max, axis=0, keepdims=True)
        shift = row_max * scale2
        ot_acc[...] = jnp.zeros_like(ot_acc)

        def value_step(step, run_sum):
            weights = jnp.exp2(s_buf[key_rows(step), :] * scale2 - shift)
            ot_acc[...] += dot_nn(v_t[:, key_rows(step)], weights.astype(jnp.bfloat16))
            return run_sum + fold(weights, jnp.sum)

        run_sum = lax.fori_loop(0, last + 1, value_step, jnp.zeros((8, width), jnp.float32))
        row_sum = jnp.sum(run_sum, axis=0, keepdims=True)
        out_t = (ot_acc[...] / row_sum).astype(jnp.bfloat16)
        row_lse = row_max * scale + jnp.log(row_sum)
        lse2 = row_lse * LOG2E
        out_f = out_t.astype(jnp.float32)
        grad_t = g_cat[...].astype(jnp.float32).T
        delta = jnp.sum(out_f * grad_t, axis=0, keepdims=True)
        out_n = out_f.T.astype(jnp.bfloat16)
        for head in range(2):
            y_ref[rows, head * dim:(head + 1) * dim] = out_n[head * BQ:(head + 1) * BQ, :]
            lse_ref[0, head:head + 1, rows] = row_lse[:, head * BQ:(head + 1) * BQ]
        dqt_acc[...] = jnp.zeros_like(dqt_acc)

        def grad_step(step, inner):
            probs = jnp.exp2(s_buf[key_rows(step), :] * scale2 - lse2)
            grad_prob = dot_nt(x_ref[key_rows(step), v_col:v_col + dim], g_cat[...])
            grad_score = (probs * (grad_prob - delta)).astype(jnp.bfloat16)
            dv_acc[key_rows(step), :] += dot_nn(probs.astype(jnp.bfloat16), g_cat[...])
            dk_acc[key_rows(step), :] += dot_nn(grad_score, q_cat[...])
            dqt_acc[...] += dot_nn(k_t[:, key_rows(step)], grad_score)
            return inner

        lax.fori_loop(0, last + 1, grad_step, 0)
        dq_n = (dqt_acc[...] * scale).T.astype(jnp.bfloat16)
        for head in range(2):
            y_ref[rows, (2 + head) * dim:(3 + head) * dim] = dq_n[head * BQ:(head + 1) * BQ, :]
        return carry

    lax.fori_loop(0, seq // BQ, query_block, 0)

    def finish(blk, carry):
        rows = pl.ds(pl.multiple_of(blk * BK, BK), BK)
        y_ref[rows, 4 * dim:5 * dim] = (dk_acc[rows, :] * scale).astype(jnp.bfloat16)
        y_ref[rows, 5 * dim:6 * dim] = dv_acc[rows, :].astype(jnp.bfloat16)
        return carry

    lax.fori_loop(0, seq // BK, finish, 0)


def attention_call(packed, source, count, prev, target, total, dim):
    seq = packed.shape[0]
    wide = 6 * dim
    pairs = count * seq * seq
    operands = [packed] + ([] if prev is None else [prev])
    return pl.pallas_call(
        attention_kernel,
        grid=(count,),
        in_specs=[pl.BlockSpec((seq, wide), lambda u: (0, source + u))] + [pl.BlockSpec(memory_space=pl.ANY)] * (len(operands) - 1),
        out_specs=[pl.BlockSpec((seq, wide), lambda u: (0, target + u)), pl.BlockSpec((1, 2, seq), lambda u: (u, 0, 0))],
        out_shape=[jax.ShapeDtypeStruct((seq, total * wide), jnp.bfloat16), jax.ShapeDtypeStruct((count, 2, seq), jnp.float32)],
        input_output_aliases={1: 0} if prev is not None else {},
        scratch_shapes=[
            pltpu.VMEM((2 * BQ, dim), jnp.bfloat16),
            pltpu.VMEM((2 * BQ, dim), jnp.bfloat16),
            pltpu.VMEM((dim, seq), jnp.bfloat16),
            pltpu.VMEM((dim, seq), jnp.bfloat16),
            pltpu.VMEM((seq, 2 * BQ), jnp.float32),
            pltpu.VMEM((dim, 2 * BQ), jnp.float32),
            pltpu.VMEM((dim, 2 * BQ), jnp.float32),
            pltpu.VMEM((seq, dim), jnp.float32),
            pltpu.VMEM((seq, dim), jnp.float32),
        ],
        compiler_params=pltpu.CompilerParams(dimension_semantics=("arbitrary",), vmem_limit_bytes=62 * 1024 * 1024),
        cost_estimate=pl.CostEstimate(flops=pairs * dim * 12, bytes_accessed=count * seq * wide * 4, transcendentals=pairs * 2),
    )(*operands)


def pack_kernel(q_ref, g_ref, k_ref, v_ref, o_ref):
    dim = q_ref.shape[-1]
    for ref, first, count in ((q_ref, 0, 2), (g_ref, 2, 2), (k_ref, 4, 1), (v_ref, 5, 1)):
        by_head = pltpu.einshape("thd->htd", ref[0])
        for head in range(ref.shape[2]):
            part, lane = divmod(head, count)
            start = (first + lane) * dim
            o_ref[part, :, start:start + dim] = by_head[head]


def unit_specs(first, parts, dim):
    def spec(count):
        return pl.BlockSpec((1, TB, parts * count, dim), lambda u, i: ((first + u) // 2, i, (first + u) % 2, 0))

    return spec(2), spec(1), pl.BlockSpec((parts, TB, 6 * dim), lambda u, i: (0, i, u))


def pack_call(queries, out_grad, keys, values, first, count, parts):
    tokens, dim = queries.shape[1], queries.shape[3]
    big, small, packed = unit_specs(first, parts, dim)
    size = parts * tokens * count * 6 * dim
    return pl.pallas_call(
        pack_kernel,
        grid=(count, tokens // TB),
        in_specs=[big, big, small, small],
        out_specs=packed,
        out_shape=jax.ShapeDtypeStruct((parts, tokens, count * 6 * dim), jnp.bfloat16),
        compiler_params=pltpu.CompilerParams(dimension_semantics=("arbitrary", "arbitrary"), vmem_limit_bytes=62 * 1024 * 1024),
        cost_estimate=pl.CostEstimate(flops=size * 200, bytes_accessed=size * 4, transcendentals=0),
    )(queries, out_grad, keys, values)


def unpack_kernel(*refs):
    y_ref = refs[0]
    o_ref, dq_ref, dk_ref, dv_ref = refs[-4:]
    dim = o_ref.shape[-1]
    for ref, first, count in ((o_ref, 0, 2), (dq_ref, 2, 2), (dk_ref, 4, 1), (dv_ref, 5, 1)):
        rows = []
        for head in range(ref.shape[2]):
            part, lane = divmod(head, count)
            start = (first + lane) * dim
            rows.append(y_ref[part, :, start:start + dim])
        ref[0] = pltpu.einshape("htd->thd", jnp.stack(rows))


def unpack_call(y, prev, first, count, shapes):
    parts, tokens = y.shape[:2]
    dim = shapes[0].shape[3]
    big, small, packed = unit_specs(first, parts, dim)
    return pl.pallas_call(
        unpack_kernel,
        grid=(count, tokens // TB),
        in_specs=[packed] + [pl.BlockSpec(memory_space=pl.ANY)] * len(prev),
        out_specs=[big, big, small, small],
        out_shape=shapes,
        input_output_aliases={i + 1: i for i in range(len(prev))},
        compiler_params=pltpu.CompilerParams(dimension_semantics=("arbitrary", "arbitrary"), vmem_limit_bytes=62 * 1024 * 1024),
        cost_estimate=pl.CostEstimate(flops=y.size * 200, bytes_accessed=y.size * 4, transcendentals=0),
    )(y, *prev)


IN_UNITS = ((0, 1), (1, 2), (3, 3))
OUT_UNITS = ((0, 3), (3, 2), (5, 1))
RUNS = ((0, 1), (1, 2), (3, 2), (5, 1))


def holder(units, unit):
    return next(idx for idx, (first, count) in enumerate(units) if first <= unit < first + count)


def solution(mesh):
    cp_size = mesh.shape["cp"]

    def attention_shard(queries, keys, values, out_grad):
        batch, tokens, heads, dim = queries.shape
        seq = cp_size * tokens
        ready = []
        for idx, (first, count) in enumerate(IN_UNITS):
            packed = pack_call(queries, out_grad, keys, values, first, count, cp_size)
            if idx:
                packed, ready[-1] = lax.optimization_barrier((packed, ready[-1]))
            ready.append(lax.all_to_all(packed, "cp", 0, 0, tiled=True))
        results, sums = {}, []
        for first, count in RUNS:
            src, dst = holder(IN_UNITS, first), holder(OUT_UNITS, first)
            results[dst], lse = attention_call(
                ready[src].reshape(seq, -1), first - IN_UNITS[src][0], count,
                results.get(dst), first - OUT_UNITS[dst][0], OUT_UNITS[dst][1], dim)
            sums.append(lse)
        done = []
        for idx in range(len(OUT_UNITS)):
            y = results[idx].reshape(cp_size, tokens, -1)
            if idx:
                y, done[-1] = lax.optimization_barrier((y, done[-1]))
            done.append(lax.all_to_all(y, "cp", 0, 0, tiled=True))
        big = jax.ShapeDtypeStruct(queries.shape, jnp.bfloat16)
        small = jax.ShapeDtypeStruct(keys.shape, jnp.bfloat16)
        outs = ()
        for idx, (first, count) in enumerate(OUT_UNITS):
            outs = unpack_call(done[idx], outs, first, count, (big, big, small, small))
        lse = jnp.concatenate(sums).reshape(batch, 2, 2, cp_size, tokens)
        lse = lax.all_to_all(jnp.transpose(lse, (3, 0, 1, 2, 4)), "cp", 0, 0, tiled=True)
        lse = jnp.transpose(lse, (1, 2, 0, 3, 4)).reshape(batch, heads, tokens)
        return outs[0], lse, outs[1], outs[2], outs[3]

    seq_spec = P("dp", "cp")
    return jax.shard_map(attention_shard, mesh=mesh, in_specs=(seq_spec, seq_spec, seq_spec, seq_spec), out_specs=(seq_spec, P("dp", None, "cp"), seq_spec, seq_spec, seq_spec), check_vma=False)
```

```python
import functools

import jax
import jax.numpy as jnp
from jax import lax
from jax.experimental import pallas as pl
from jax.experimental.pallas import tpu as pltpu
from jax.sharding import PartitionSpec as P


LOG2E = 1.4426950408889634
BQ = 256
BK = 512
TB = 64


def dot_nt(lhs, rhs):
    return lax.dot_general(lhs, rhs, (((1,), (1,)), ((), ())), preferred_element_type=jnp.float32)


def dot_nn(lhs, rhs):
    return lax.dot_general(lhs, rhs, (((1,), (0,)), ((), ())), preferred_element_type=jnp.float32)


def attention_kernel(x_ref, *refs):
    y_ref, lse_ref, q_cat, g_cat, k_t, v_t, s_even, s_odd, ot_acc, dqt_acc, dk_acc, dv_acc = refs[-12:]
    seq = x_ref.shape[0]
    dim = k_t.shape[0]
    width = 2 * BQ
    scale = dim ** -0.5
    scale2 = scale * LOG2E
    q_col, g_col, k_col, v_col = 0, 2 * dim, 4 * dim, 5 * dim

    def prepare(blk, carry):
        rows = pl.ds(pl.multiple_of(blk * BK, BK), BK)
        k_t[:, rows] = x_ref[rows, k_col:k_col + dim].T
        v_t[:, rows] = x_ref[rows, v_col:v_col + dim].T
        dk_acc[rows, :] = jnp.zeros((BK, dim), jnp.float32)
        dv_acc[rows, :] = jnp.zeros((BK, dim), jnp.float32)
        return carry

    lax.fori_loop(0, seq // BK, prepare, 0)

    def fold(tile, op):
        return op(tile.reshape(BK // 8, 8, width), axis=0)

    def query_block(blk, carry):
        rows = pl.ds(pl.multiple_of(blk * BQ, BQ), BQ)
        for head in range(2):
            q_cat[head * BQ:(head + 1) * BQ, :] = x_ref[rows, q_col + head * dim:q_col + (head + 1) * dim]
            g_cat[head * BQ:(head + 1) * BQ, :] = x_ref[rows, g_col + head * dim:g_col + (head + 1) * dim]
        last = (blk * BQ) // BK

        def key_rows(step):
            return pl.ds(pl.multiple_of(step * BK, BK), BK)

        def slot(idx):
            return pl.ds(pl.multiple_of(idx * BK, BK), BK)

        def absorb(src, idx, step, carry):
            acc_max, run_max, run_sum = carry
            alpha = jnp.exp2((acc_max - run_max) * scale2)
            weights = jnp.exp2(src[slot(idx), :] * scale2 - run_max * scale2)
            ot_acc[...] = ot_acc[...] * alpha + dot_nn(v_t[:, key_rows(step)], weights.astype(jnp.bfloat16))
            return run_sum * alpha + fold(weights, jnp.sum)

        def advance(dst, idx, step, src, src_idx, src_step, carry):
            scores = dot_nt(x_ref[key_rows(step), k_col:k_col + dim], q_cat[...])
            dst[slot(idx), :] = scores
            new_max = jnp.maximum(carry[1], jnp.max(fold(scores, jnp.max), axis=0, keepdims=True))
            run_sum = absorb(src, src_idx, src_step, carry)
            return carry[1], new_max, run_sum

        def before(pair):
            return jnp.where(pair == 0, last, 2 * pair - 1)

        def score_pair(pair, carry):
            carry = advance(s_even, pair, 2 * pair, s_odd, pair, before(pair), carry)
            return advance(s_odd, pair + 1, 2 * pair + 1, s_even, pair, 2 * pair, carry)

        half = last // 2

        def finish_even(carry):
            carry = advance(s_even, half, 2 * half, s_odd, half, before(half), carry)
            return carry[1], absorb(s_even, half, 2 * half, carry)

        def finish_odd(carry):
            return carry[1], absorb(s_odd, half, before(half), carry)

        scores = dot_nt(x_ref[key_rows(last), k_col:k_col + dim], q_cat[...])
        key_pos = last * BK + lax.broadcasted_iota(jnp.int32, (BK, width), 0)
        query_pos = blk * BQ + lax.broadcasted_iota(jnp.int32, (BK, width), 1) % BQ
        scores = jnp.where(key_pos <= query_pos, scores, -jnp.inf)
        s_odd[slot(0), :] = scores
        row_max = jnp.max(fold(scores, jnp.max), axis=0, keepdims=True)
        ot_acc[...] = jnp.zeros_like(ot_acc)
        state = lax.fori_loop(0, half, score_pair, (row_max, row_max, jnp.zeros((8, width), jnp.float32)))
        row_max, run_sum = lax.cond(last % 2 == 1, finish_even, finish_odd, state)
        row_sum = jnp.sum(run_sum, axis=0, keepdims=True)
        out_t = (ot_acc[...] / row_sum).astype(jnp.bfloat16)
        row_lse = row_max * scale + jnp.log(row_sum)
        lse2 = row_lse * LOG2E
        out_f = out_t.astype(jnp.float32)
        grad_t = g_cat[...].astype(jnp.float32).T
        delta = jnp.sum(out_f * grad_t, axis=0, keepdims=True)
        out_n = out_f.T.astype(jnp.bfloat16)
        for head in range(2):
            y_ref[rows, head * dim:(head + 1) * dim] = out_n[head * BQ:(head + 1) * BQ, :]
            lse_ref[0, head:head + 1, rows] = row_lse[:, head * BQ:(head + 1) * BQ]
        dqt_acc[...] = jnp.zeros_like(dqt_acc)

        def grad_step(src, idx, step):
            probs = jnp.exp2(src[slot(idx), :] * scale2 - lse2)
            grad_prob = dot_nt(x_ref[key_rows(step), v_col:v_col + dim], g_cat[...])
            grad_score = (probs * (grad_prob - delta)).astype(jnp.bfloat16)
            dv_acc[key_rows(step), :] += dot_nn(probs.astype(jnp.bfloat16), g_cat[...])
            dk_acc[key_rows(step), :] += dot_nn(grad_score, q_cat[...])
            dqt_acc[...] += dot_nn(k_t[:, key_rows(step)], grad_score)

        def grad_pair(pair, inner):
            grad_step(s_odd, pair, before(pair))
            grad_step(s_even, pair, 2 * pair)
            return inner

        lax.fori_loop(0, (last + 1) // 2, grad_pair, 0)

        @pl.when(last % 2 == 0)
        def _():
            grad_step(s_odd, half, before(half))

        dq_n = (dqt_acc[...] * scale).T.astype(jnp.bfloat16)
        for head in range(2):
            y_ref[rows, (2 + head) * dim:(3 + head) * dim] = dq_n[head * BQ:(head + 1) * BQ, :]
        return carry

    lax.fori_loop(0, seq // BQ, query_block, 0)

    def finish(blk, carry):
        rows = pl.ds(pl.multiple_of(blk * BK, BK), BK)
        y_ref[rows, 4 * dim:5 * dim] = (dk_acc[rows, :] * scale).astype(jnp.bfloat16)
        y_ref[rows, 5 * dim:6 * dim] = dv_acc[rows, :].astype(jnp.bfloat16)
        return carry

    lax.fori_loop(0, seq // BK, finish, 0)


def attention_scratch(seq, dim):
    return [
        pltpu.VMEM((2 * BQ, dim), jnp.bfloat16),
        pltpu.VMEM((2 * BQ, dim), jnp.bfloat16),
        pltpu.VMEM((dim, seq), jnp.bfloat16),
        pltpu.VMEM((dim, seq), jnp.bfloat16),
        pltpu.VMEM((seq // 2, 2 * BQ), jnp.float32),
        pltpu.VMEM((seq // 2, 2 * BQ), jnp.float32),
        pltpu.VMEM((dim, 2 * BQ), jnp.float32),
        pltpu.VMEM((dim, 2 * BQ), jnp.float32),
        pltpu.VMEM((seq, dim), jnp.float32),
        pltpu.VMEM((seq, dim), jnp.float32),
    ]


def pack_kernel(q_ref, g_ref, k_ref, v_ref, o_ref):
    dim = q_ref.shape[-1]
    for ref, first, count in ((q_ref, 0, 2), (g_ref, 2, 2), (k_ref, 4, 1), (v_ref, 5, 1)):
        by_head = pltpu.einshape("thd->htd", ref[0])
        for head in range(ref.shape[2]):
            part, lane = divmod(head, count)
            start = (first + lane) * dim
            o_ref[part, :, start:start + dim] = by_head[head]


def unit_specs(first, parts, dim, skip=0):
    def spec(count):
        return pl.BlockSpec((1, TB, parts * count, dim), lambda u, i: ((first + u) // 2, skip + i, (first + u) % 2, 0))

    return spec(2), spec(1), pl.BlockSpec((parts, TB, 6 * dim), lambda u, i: (0, i, u))


def unpack_kernel(*refs):
    y_ref = refs[0]
    o_ref, dq_ref, dk_ref, dv_ref = refs[-4:]
    dim = o_ref.shape[-1]
    for ref, first, count in ((o_ref, 0, 2), (dq_ref, 2, 2), (dk_ref, 4, 1), (dv_ref, 5, 1)):
        rows = []
        for head in range(ref.shape[2]):
            part, lane = divmod(head, count)
            start = (first + lane) * dim
            rows.append(y_ref[part, :, start:start + dim])
        ref[0] = pltpu.einshape("htd->thd", jnp.stack(rows))


def peer_rows(offset, tokens, piece=0, pieces=1):
    size = tokens // pieces
    start = jnp.bitwise_xor(lax.axis_index("cp"), offset) * tokens + piece * size
    return pl.ds(pl.multiple_of(start, size), size)


def attention_split_kernel(split_in, split_out, parts, *refs):
    count_in, count_out = (parts if split_in else 1), parts * split_out
    ins, outs, lse_ref = refs[:count_in], refs[count_in:count_in + count_out], refs[count_in + count_out]
    scratch = refs[count_in + count_out + 1:]
    x_ref, y_ref, sems = scratch[-3:]
    tokens = x_ref.shape[0] // parts
    if split_in:
        copies = [pltpu.make_async_copy(ref, x_ref.at[peer_rows(k, tokens)], sems.at[k]) for k, ref in enumerate(ins)]
    else:
        copies = [pltpu.make_async_copy(ins[0], x_ref, sems.at[0])]
    for copy in copies:
        copy.start()
    for copy in copies:
        copy.wait()
    attention_kernel(x_ref, y_ref, lse_ref, *scratch[:-3])
    copies = [
        pltpu.make_async_copy(y_ref.at[peer_rows(idx % parts, tokens, idx // parts, split_out)], ref, sems.at[idx])
        for idx, ref in enumerate(outs)
    ]
    for copy in copies:
        copy.start()
    for copy in copies:
        copy.wait()


def attention_split_call(ins, split_out, parts, seq, dim):
    wide = 6 * dim
    split_in = len(ins) > 1
    pairs = seq * seq
    any_spec = pl.BlockSpec(memory_space=pl.ANY)
    y_shapes = [jax.ShapeDtypeStruct((seq // parts // split_out, wide), jnp.bfloat16)] * (parts * split_out)
    res = pl.pallas_call(
        functools.partial(attention_split_kernel, split_in, split_out, parts),
        in_specs=[any_spec] * len(ins),
        out_specs=[any_spec] * len(y_shapes) + [pl.BlockSpec(memory_space=pltpu.VMEM)],
        out_shape=y_shapes + [jax.ShapeDtypeStruct((1, 2, seq), jnp.float32)],
        scratch_shapes=attention_scratch(seq, dim) + [
            pltpu.VMEM((seq, wide), jnp.bfloat16),
            pltpu.VMEM((seq, wide), jnp.bfloat16),
            pltpu.SemaphoreType.DMA((2 * parts,)),
        ],
        compiler_params=pltpu.CompilerParams(vmem_limit_bytes=62 * 1024 * 1024),
        cost_estimate=pl.CostEstimate(flops=pairs * dim * 12, bytes_accessed=seq * wide * 4, transcendentals=pairs * 2),
    )(*ins)
    return res[:-1], res[-1]


def pack_split_kernel(q_ref, g_ref, k_ref, v_ref, *refs):
    *outs, buf = refs
    pack_kernel(q_ref, g_ref, k_ref, v_ref, buf)
    for k, ref in enumerate(outs):
        ref[...] = buf[jnp.bitwise_xor(lax.axis_index("cp"), k)]


def pack_split_call(queries, out_grad, keys, values, unit, parts):
    tokens, dim = queries.shape[1], queries.shape[3]
    big, small, _ = unit_specs(unit, parts, dim)
    wide = 6 * dim
    size = parts * tokens * wide
    return pl.pallas_call(
        pack_split_kernel,
        grid=(1, tokens // TB),
        in_specs=[big, big, small, small],
        out_specs=[pl.BlockSpec((TB, wide), lambda u, i: (i, 0))] * parts,
        out_shape=[jax.ShapeDtypeStruct((tokens, wide), jnp.bfloat16)] * parts,
        scratch_shapes=[pltpu.VMEM((parts, TB, wide), jnp.bfloat16)],
        compiler_params=pltpu.CompilerParams(dimension_semantics=("arbitrary", "arbitrary"), vmem_limit_bytes=62 * 1024 * 1024),
        cost_estimate=pl.CostEstimate(flops=size * 200, bytes_accessed=size * 4, transcendentals=0),
    )(queries, out_grad, keys, values)


def unpack_split_kernel(parts, *refs):
    buf = refs[-1]
    for k in range(parts):
        buf[jnp.bitwise_xor(lax.axis_index("cp"), k)] = refs[k][...]
    unpack_kernel(buf, *refs[parts:-1])


def unpack_split_call(chunks, prev, unit, piece, shapes):
    parts = len(chunks)
    tokens, wide = chunks[0].shape
    dim = shapes[0].shape[3]
    big, small, _ = unit_specs(unit, parts, dim, piece * tokens // TB)
    size = parts * tokens * wide
    return pl.pallas_call(
        functools.partial(unpack_split_kernel, parts),
        grid=(1, tokens // TB),
        in_specs=[pl.BlockSpec((TB, wide), lambda u, i: (i, 0))] * parts + [pl.BlockSpec(memory_space=pl.ANY)] * len(prev),
        out_specs=[big, big, small, small],
        out_shape=shapes,
        input_output_aliases={i + parts: i for i in range(len(prev))},
        scratch_shapes=[pltpu.VMEM((parts, TB, wide), jnp.bfloat16)],
        compiler_params=pltpu.CompilerParams(dimension_semantics=("arbitrary", "arbitrary"), vmem_limit_bytes=62 * 1024 * 1024),
        cost_estimate=pl.CostEstimate(flops=size * 200, bytes_accessed=size * 4, transcendentals=0),
    )(*chunks, *prev)


def lse_split_kernel(counts, *refs):
    ins, outs = refs[:len(counts)], refs[len(counts):]
    tokens = outs[0].shape[1]
    for k, out in enumerate(outs):
        row = 0
        for ref, count in zip(ins, counts):
            for unit in range(count):
                out[row:row + 2, :] = ref[unit, :, peer_rows(k, tokens)]
                row += 2


def lse_join_kernel(*refs):
    *ins, out = refs
    batch = out.shape[0]
    parts = len(ins)
    for k, ref in enumerate(ins):
        peer = jnp.bitwise_xor(lax.axis_index("cp"), k)
        for row in range(4 * batch):
            group, lane = divmod(row % 4, 2)
            out[row // 4, pl.ds(2 * parts * group + 2 * peer + lane, 1), :] = ref[row:row + 1, :]


def lse_split_call(sums, parts):
    rows = 2 * sum(arr.shape[0] for arr in sums)
    tokens = sums[0].shape[2] // parts
    vmem = pl.BlockSpec(memory_space=pltpu.VMEM)
    return pl.pallas_call(
        functools.partial(lse_split_kernel, [arr.shape[0] for arr in sums]),
        in_specs=[vmem] * len(sums),
        out_specs=[vmem] * parts,
        out_shape=[jax.ShapeDtypeStruct((rows, tokens), jnp.float32)] * parts,
        cost_estimate=pl.CostEstimate(flops=10 ** 7, bytes_accessed=rows * tokens * parts * 8, transcendentals=0),
    )(*sums)


def lse_join_call(chunks, batch):
    rows, tokens = chunks[0].shape
    vmem = pl.BlockSpec(memory_space=pltpu.VMEM)
    return pl.pallas_call(
        lse_join_kernel,
        in_specs=[vmem] * len(chunks),
        out_specs=vmem,
        out_shape=jax.ShapeDtypeStruct((batch, rows * len(chunks) // batch, tokens), jnp.float32),
        cost_estimate=pl.CostEstimate(flops=10 ** 7, bytes_accessed=rows * tokens * len(chunks) * 8, transcendentals=0),
    )(*chunks)


def exchange(chunks):
    size = len(chunks)
    out = [chunks[0]]
    for offset in range(1, size):
        pairs = [(rank, rank ^ offset) for rank in range(size)]
        out.append(lax.ppermute(chunks[offset], "cp", pairs))
    return out


TAIL = 2


def solution(mesh):
    cp_size = mesh.shape["cp"]

    def attention_shard(queries, keys, values, out_grad):
        batch, tokens, _, dim = queries.shape
        units = 2 * batch
        ys, sums = [], []
        for unit in range(units):
            packed = pack_split_call(queries, out_grad, keys, values, unit, cp_size)
            ready = exchange(packed)
            y, lse = attention_split_call(ready, TAIL if unit == units - 1 else 1, cp_size, cp_size * tokens, dim)
            ys.append(y)
            sums.append(lse)
        lse = lse_split_call(sums, cp_size)
        lse = exchange(lse)
        lse = lse_join_call(lse, batch)
        big = jax.ShapeDtypeStruct(queries.shape, jnp.bfloat16)
        small = jax.ShapeDtypeStruct(keys.shape, jnp.bfloat16)
        outs = ()
        for unit, y in enumerate(ys):
            for piece in range(len(y) // cp_size):
                chunks = exchange(y[piece * cp_size:(piece + 1) * cp_size])
                outs = unpack_split_call(chunks, outs, unit, piece, (big, big, small, small))
        return outs[0], lse, outs[1], outs[2], outs[3]

    seq_spec = P("dp", "cp")
    return jax.shard_map(attention_shard, mesh=mesh, in_specs=(seq_spec, seq_spec, seq_spec, seq_spec), out_specs=(seq_spec, P("dp", None, "cp"), seq_spec, seq_spec, seq_spec), check_vma=False)
```

```python
import functools

import jax
import jax.numpy as jnp
from jax import lax
from jax.experimental import pallas as pl
from jax.experimental.pallas import tpu as pltpu
from jax.sharding import PartitionSpec as P


LOG2E = 1.4426950408889634
BQ = 256
BK = 512
TB = 64


def dot_nt(lhs, rhs):
    return lax.dot_general(lhs, rhs, (((1,), (1,)), ((), ())), preferred_element_type=jnp.float32)


def dot_nn(lhs, rhs):
    return lax.dot_general(lhs, rhs, (((1,), (0,)), ((), ())), preferred_element_type=jnp.float32)


def attention_kernel(x_ref, *refs):
    y_ref, lse_ref, q_cat, g_cat, k_t, v_t, s_even, s_odd, ot_acc, dqt_acc, dk_acc, dv_acc = refs[-12:]
    seq = x_ref.shape[0]
    dim = k_t.shape[0]
    width = 2 * BQ
    scale = dim ** -0.5
    scale2 = scale * LOG2E
    q_col, g_col, k_col, v_col = 0, 2 * dim, 4 * dim, 5 * dim

    def prepare(blk, carry):
        rows = pl.ds(pl.multiple_of(blk * BK, BK), BK)
        k_t[:, rows] = x_ref[rows, k_col:k_col + dim].T
        v_t[:, rows] = x_ref[rows, v_col:v_col + dim].T
        dk_acc[rows, :] = jnp.zeros((BK, dim), jnp.float32)
        dv_acc[rows, :] = jnp.zeros((BK, dim), jnp.float32)
        return carry

    lax.fori_loop(0, seq // BK, prepare, 0)

    def fold(tile, op):
        return op(tile.reshape(BK // 8, 8, width), axis=0)

    def query_block(blk, carry):
        rows = pl.ds(pl.multiple_of(blk * BQ, BQ), BQ)
        for head in range(2):
            q_cat[head * BQ:(head + 1) * BQ, :] = x_ref[rows, q_col + head * dim:q_col + (head + 1) * dim]
            g_cat[head * BQ:(head + 1) * BQ, :] = x_ref[rows, g_col + head * dim:g_col + (head + 1) * dim]
        last = (blk * BQ) // BK

        def key_rows(step):
            return pl.ds(pl.multiple_of(step * BK, BK), BK)

        def slot(idx):
            return pl.ds(pl.multiple_of(idx * BK, BK), BK)

        def absorb(src, idx, step, carry):
            acc_max, run_max, run_sum = carry
            alpha = jnp.exp2((acc_max - run_max) * scale2)
            weights = jnp.exp2(src[slot(idx), :] * scale2 - run_max * scale2)
            ot_acc[...] = ot_acc[...] * alpha + dot_nn(v_t[:, key_rows(step)], weights.astype(jnp.bfloat16))
            return run_sum * alpha + fold(weights, jnp.sum)

        def advance(dst, idx, step, src, src_idx, src_step, carry):
            scores = dot_nt(x_ref[key_rows(step), k_col:k_col + dim], q_cat[...])
            dst[slot(idx), :] = scores
            new_max = jnp.maximum(carry[1], jnp.max(fold(scores, jnp.max), axis=0, keepdims=True))
            run_sum = absorb(src, src_idx, src_step, carry)
            return carry[1], new_max, run_sum

        def before(pair):
            return jnp.where(pair == 0, last, 2 * pair - 1)

        def score_pair(pair, carry):
            carry = advance(s_even, pair, 2 * pair, s_odd, pair, before(pair), carry)
            return advance(s_odd, pair + 1, 2 * pair + 1, s_even, pair, 2 * pair, carry)

        half = last // 2

        def finish_even(carry):
            carry = advance(s_even, half, 2 * half, s_odd, half, before(half), carry)
            return carry[1], absorb(s_even, half, 2 * half, carry)

        def finish_odd(carry):
            return carry[1], absorb(s_odd, half, before(half), carry)

        scores = dot_nt(x_ref[key_rows(last), k_col:k_col + dim], q_cat[...])
        key_pos = last * BK + lax.broadcasted_iota(jnp.int32, (BK, width), 0)
        query_pos = blk * BQ + lax.broadcasted_iota(jnp.int32, (BK, width), 1) % BQ
        scores = jnp.where(key_pos <= query_pos, scores, -jnp.inf)
        s_odd[slot(0), :] = scores
        row_max = jnp.max(fold(scores, jnp.max), axis=0, keepdims=True)
        ot_acc[...] = jnp.zeros_like(ot_acc)
        state = lax.fori_loop(0, half, score_pair, (row_max, row_max, jnp.zeros((8, width), jnp.float32)))
        row_max, run_sum = lax.cond(last % 2 == 1, finish_even, finish_odd, state)
        row_sum = jnp.sum(run_sum, axis=0, keepdims=True)
        out_t = (ot_acc[...] / row_sum).astype(jnp.bfloat16)
        row_lse = row_max * scale + jnp.log(row_sum)
        lse2 = row_lse * LOG2E
        out_f = out_t.astype(jnp.float32)
        grad_t = g_cat[...].astype(jnp.float32).T
        delta = jnp.sum(out_f * grad_t, axis=0, keepdims=True)
        out_n = out_f.T.astype(jnp.bfloat16)
        for head in range(2):
            y_ref[rows, head * dim:(head + 1) * dim] = out_n[head * BQ:(head + 1) * BQ, :]
            lse_ref[0, head:head + 1, rows] = row_lse[:, head * BQ:(head + 1) * BQ]
        dqt_acc[...] = jnp.zeros_like(dqt_acc)

        def grad_step(src, idx, step):
            probs = jnp.exp2(src[slot(idx), :] * scale2 - lse2)
            grad_prob = dot_nt(x_ref[key_rows(step), v_col:v_col + dim], g_cat[...])
            grad_score = (probs * (grad_prob - delta)).astype(jnp.bfloat16)
            dv_acc[key_rows(step), :] += dot_nn(probs.astype(jnp.bfloat16), g_cat[...])
            dk_acc[key_rows(step), :] += dot_nn(grad_score, q_cat[...])
            dqt_acc[...] += dot_nn(k_t[:, key_rows(step)], grad_score)

        def grad_pair(pair, inner):
            grad_step(s_odd, pair, before(pair))
            grad_step(s_even, pair, 2 * pair)
            return inner

        lax.fori_loop(0, (last + 1) // 2, grad_pair, 0)

        @pl.when(last % 2 == 0)
        def _():
            grad_step(s_odd, half, before(half))

        dq_n = (dqt_acc[...] * scale).T.astype(jnp.bfloat16)
        for head in range(2):
            y_ref[rows, (2 + head) * dim:(3 + head) * dim] = dq_n[head * BQ:(head + 1) * BQ, :]
        return carry

    lax.fori_loop(0, seq // BQ, query_block, 0)

    def finish(blk, carry):
        rows = pl.ds(pl.multiple_of(blk * BK, BK), BK)
        y_ref[rows, 4 * dim:5 * dim] = (dk_acc[rows, :] * scale).astype(jnp.bfloat16)
        y_ref[rows, 5 * dim:6 * dim] = dv_acc[rows, :].astype(jnp.bfloat16)
        return carry

    lax.fori_loop(0, seq // BK, finish, 0)


def attention_scratch(seq, dim):
    return [
        pltpu.VMEM((2 * BQ, dim), jnp.bfloat16),
        pltpu.VMEM((2 * BQ, dim), jnp.bfloat16),
        pltpu.VMEM((dim, seq), jnp.bfloat16),
        pltpu.VMEM((dim, seq), jnp.bfloat16),
        pltpu.VMEM((seq // 2, 2 * BQ), jnp.float32),
        pltpu.VMEM((seq // 2, 2 * BQ), jnp.float32),
        pltpu.VMEM((dim, 2 * BQ), jnp.float32),
        pltpu.VMEM((dim, 2 * BQ), jnp.float32),
        pltpu.VMEM((seq, dim), jnp.float32),
        pltpu.VMEM((seq, dim), jnp.float32),
    ]


def pack_kernel(q_ref, g_ref, k_ref, v_ref, o_ref):
    dim = q_ref.shape[-1]
    for ref, first, count in ((q_ref, 0, 2), (g_ref, 2, 2), (k_ref, 4, 1), (v_ref, 5, 1)):
        by_head = pltpu.einshape("thd->htd", ref[0])
        for head in range(ref.shape[2]):
            part, lane = divmod(head, count)
            start = (first + lane) * dim
            o_ref[part, :, start:start + dim] = by_head[head]


def unit_specs(first, parts, dim, skip=0):
    def spec(count):
        return pl.BlockSpec((1, TB, parts * count, dim), lambda u, i: ((first + u) // 2, skip + i, (first + u) % 2, 0))

    return spec(2), spec(1), pl.BlockSpec((parts, TB, 6 * dim), lambda u, i: (0, i, u))


def unpack_kernel(*refs):
    y_ref = refs[0]
    o_ref, dq_ref, dk_ref, dv_ref = refs[-4:]
    dim = o_ref.shape[-1]
    for ref, first, count in ((o_ref, 0, 2), (dq_ref, 2, 2), (dk_ref, 4, 1), (dv_ref, 5, 1)):
        rows = []
        for head in range(ref.shape[2]):
            part, lane = divmod(head, count)
            start = (first + lane) * dim
            rows.append(y_ref[part, :, start:start + dim])
        ref[0] = pltpu.einshape("htd->thd", jnp.stack(rows))


def peer_rows(offset, tokens, piece=0, pieces=1):
    size = tokens // pieces
    start = jnp.bitwise_xor(lax.axis_index("cp"), offset) * tokens + piece * size
    return pl.ds(pl.multiple_of(start, size), size)


def attention_split_kernel(split_in, split_out, parts, *refs):
    count_in, count_out = parts * split_in, parts * split_out
    ins, outs, lse_ref = refs[:count_in], refs[count_in:count_in + count_out], refs[count_in + count_out]
    scratch = refs[count_in + count_out + 1:]
    x_ref, y_ref, sems = scratch[-3:]
    tokens = x_ref.shape[0] // parts
    copies = [
        pltpu.make_async_copy(ref, x_ref.at[peer_rows(idx % parts, tokens, idx // parts, split_in)], sems.at[idx])
        for idx, ref in enumerate(ins)
    ]
    for copy in copies:
        copy.start()
    for copy in copies:
        copy.wait()
    attention_kernel(x_ref, y_ref, lse_ref, *scratch[:-3])
    copies = [
        pltpu.make_async_copy(y_ref.at[peer_rows(idx % parts, tokens, idx // parts, split_out)], ref, sems.at[idx])
        for idx, ref in enumerate(outs)
    ]
    for copy in copies:
        copy.start()
    for copy in copies:
        copy.wait()


def attention_split_call(ins, split_out, parts, seq, dim):
    wide = 6 * dim
    split_in = len(ins) // parts
    pairs = seq * seq
    any_spec = pl.BlockSpec(memory_space=pl.ANY)
    y_shapes = [jax.ShapeDtypeStruct((seq // parts // split_out, wide), jnp.bfloat16)] * (parts * split_out)
    res = pl.pallas_call(
        functools.partial(attention_split_kernel, split_in, split_out, parts),
        in_specs=[any_spec] * len(ins),
        out_specs=[any_spec] * len(y_shapes) + [pl.BlockSpec(memory_space=pltpu.VMEM)],
        out_shape=y_shapes + [jax.ShapeDtypeStruct((1, 2, seq), jnp.float32)],
        scratch_shapes=attention_scratch(seq, dim) + [
            pltpu.VMEM((seq, wide), jnp.bfloat16),
            pltpu.VMEM((seq, wide), jnp.bfloat16),
            pltpu.SemaphoreType.DMA((3 * parts,)),
        ],
        compiler_params=pltpu.CompilerParams(vmem_limit_bytes=62 * 1024 * 1024),
        cost_estimate=pl.CostEstimate(flops=pairs * dim * 12, bytes_accessed=seq * wide * 4, transcendentals=pairs * 2),
    )(*ins)
    return res[:-1], res[-1]


def pack_split_kernel(q_ref, g_ref, k_ref, v_ref, *refs):
    *outs, buf = refs
    pack_kernel(q_ref, g_ref, k_ref, v_ref, buf)
    for k, ref in enumerate(outs):
        ref[...] = buf[jnp.bitwise_xor(lax.axis_index("cp"), k)]


def pack_split_call(queries, out_grad, keys, values, unit, piece, pieces, parts):
    tokens, dim = queries.shape[1] // pieces, queries.shape[3]
    big, small, _ = unit_specs(unit, parts, dim, piece * tokens // TB)
    wide = 6 * dim
    size = parts * tokens * wide
    return pl.pallas_call(
        pack_split_kernel,
        grid=(1, tokens // TB),
        in_specs=[big, big, small, small],
        out_specs=[pl.BlockSpec((TB, wide), lambda u, i: (i, 0))] * parts,
        out_shape=[jax.ShapeDtypeStruct((tokens, wide), jnp.bfloat16)] * parts,
        scratch_shapes=[pltpu.VMEM((parts, TB, wide), jnp.bfloat16)],
        compiler_params=pltpu.CompilerParams(dimension_semantics=("arbitrary", "arbitrary"), vmem_limit_bytes=62 * 1024 * 1024),
        cost_estimate=pl.CostEstimate(flops=size * 200, bytes_accessed=size * 4, transcendentals=0),
    )(queries, out_grad, keys, values)


def unpack_split_kernel(parts, *refs):
    buf = refs[-1]
    for k in range(parts):
        buf[jnp.bitwise_xor(lax.axis_index("cp"), k)] = refs[k][...]
    unpack_kernel(buf, *refs[parts:-1])


def unpack_split_call(chunks, prev, unit, piece, shapes):
    parts = len(chunks)
    tokens, wide = chunks[0].shape
    dim = shapes[0].shape[3]
    big, small, _ = unit_specs(unit, parts, dim, piece * tokens // TB)
    size = parts * tokens * wide
    return pl.pallas_call(
        functools.partial(unpack_split_kernel, parts),
        grid=(1, tokens // TB),
        in_specs=[pl.BlockSpec((TB, wide), lambda u, i: (i, 0))] * parts + [pl.BlockSpec(memory_space=pl.ANY)] * len(prev),
        out_specs=[big, big, small, small],
        out_shape=shapes,
        input_output_aliases={i + parts: i for i in range(len(prev))},
        scratch_shapes=[pltpu.VMEM((parts, TB, wide), jnp.bfloat16)],
        compiler_params=pltpu.CompilerParams(dimension_semantics=("arbitrary", "arbitrary"), vmem_limit_bytes=62 * 1024 * 1024),
        cost_estimate=pl.CostEstimate(flops=size * 200, bytes_accessed=size * 4, transcendentals=0),
    )(*chunks, *prev)


def lse_split_kernel(counts, *refs):
    ins, outs = refs[:len(counts)], refs[len(counts):]
    tokens = outs[0].shape[1]
    for k, out in enumerate(outs):
        row = 0
        for ref, count in zip(ins, counts):
            for unit in range(count):
                out[row:row + 2, :] = ref[unit, :, peer_rows(k, tokens)]
                row += 2


def lse_join_kernel(*refs):
    *ins, out = refs
    batch = out.shape[0]
    parts = len(ins)
    for k, ref in enumerate(ins):
        peer = jnp.bitwise_xor(lax.axis_index("cp"), k)
        for row in range(4 * batch):
            group, lane = divmod(row % 4, 2)
            out[row // 4, pl.ds(2 * parts * group + 2 * peer + lane, 1), :] = ref[row:row + 1, :]


def lse_split_call(sums, parts):
    rows = 2 * sum(arr.shape[0] for arr in sums)
    tokens = sums[0].shape[2] // parts
    vmem = pl.BlockSpec(memory_space=pltpu.VMEM)
    return pl.pallas_call(
        functools.partial(lse_split_kernel, [arr.shape[0] for arr in sums]),
        in_specs=[vmem] * len(sums),
        out_specs=[vmem] * parts,
        out_shape=[jax.ShapeDtypeStruct((rows, tokens), jnp.float32)] * parts,
        cost_estimate=pl.CostEstimate(flops=10 ** 7, bytes_accessed=rows * tokens * parts * 8, transcendentals=0),
    )(*sums)


def lse_join_call(chunks, batch):
    rows, tokens = chunks[0].shape
    vmem = pl.BlockSpec(memory_space=pltpu.VMEM)
    return pl.pallas_call(
        lse_join_kernel,
        in_specs=[vmem] * len(chunks),
        out_specs=vmem,
        out_shape=jax.ShapeDtypeStruct((batch, rows * len(chunks) // batch, tokens), jnp.float32),
        cost_estimate=pl.CostEstimate(flops=10 ** 7, bytes_accessed=rows * tokens * len(chunks) * 8, transcendentals=0),
    )(*chunks)


def exchange(chunks):
    size = len(chunks)
    out = [chunks[0]]
    for offset in range(1, size):
        pairs = [(rank, rank ^ offset) for rank in range(size)]
        out.append(lax.ppermute(chunks[offset], "cp", pairs))
    return out


HEAD = 2
TAIL = 3


def solution(mesh):
    cp_size = mesh.shape["cp"]

    def attention_shard(queries, keys, values, out_grad):
        batch, tokens, _, dim = queries.shape
        units = 2 * batch
        ys, sums = [], []
        for unit in range(units):
            ready = []
            pieces = HEAD if unit == 0 else 1
            for piece in range(pieces):
                packed = pack_split_call(queries, out_grad, keys, values, unit, piece, pieces, cp_size)
                ready += exchange(packed)
            y, lse = attention_split_call(ready, TAIL if unit == units - 1 else 1, cp_size, cp_size * tokens, dim)
            ys.append(y)
            sums.append(lse)
        lse = lse_split_call(sums, cp_size)
        lse = exchange(lse)
        lse = lse_join_call(lse, batch)
        big = jax.ShapeDtypeStruct(queries.shape, jnp.bfloat16)
        small = jax.ShapeDtypeStruct(keys.shape, jnp.bfloat16)
        outs = ()
        for unit, y in enumerate(ys):
            for piece in range(len(y) // cp_size):
                chunks = exchange(y[piece * cp_size:(piece + 1) * cp_size])
                outs = unpack_split_call(chunks, outs, unit, piece, (big, big, small, small))
        return outs[0], lse, outs[1], outs[2], outs[3]

    seq_spec = P("dp", "cp")
    return jax.shard_map(attention_shard, mesh=mesh, in_specs=(seq_spec, seq_spec, seq_spec, seq_spec), out_specs=(seq_spec, P("dp", None, "cp"), seq_spec, seq_spec, seq_spec), check_vma=False)
```
